32 devices in a mesh: dp: 32 (over z, y, x, core), tensor: 1.
Axes of the slice: x: 2, y: 2, z: 4, core: 2. Of those that a mesh axis runs over, the one named last changes fastest.
Arguments:
- latent_raw: bfloat16 [6144, 512], P('dp'), may hold values from -6 to 6
- norm_gain: float32 [512], replicated, may hold values from 0.5 to 1.5
- up_weight: bfloat16 [512, 4096], P(None, 'tensor'), may hold values from -0.25 to 0.25
- grad_kv: bfloat16 [6144, 4096], P('dp', 'tensor'), may hold values from -3 to 3
Outputs:
- latent_grad: bfloat16 [6144, 512], P('dp')
- gain_grad: float32 [512], replicated
- weight_grad: float32 [512, 4096], P('dp', 'tensor')
The draws below stay inside these ranges and needn't reach their ends.
All inputs are finite; a program needn't handle non-finite values.
Results may differ from the reference program's by a relative error of at most 0.0029.
Values may be sent and summed in bfloat16 or wider, within the bound.
A program may use at most 64 MiB of HBM per device.

```python
import jax
import jax.numpy as jnp
from jax import lax

KVL = 512
HEAD_DIM = 128
HEADS = 16
TOKENS = 6144


def strengthened(drawn, rng, source, target, blocks, factor):
    owner, partner = [(jnp.arange(drawn.shape[position]) // (drawn.shape[position] // blocks)).reshape([-1 if axis == position else 1 for axis in range(drawn.ndim)]) for position in (source, target)]
    chosen = jax.random.permutation(rng, blocks)[partner]
    strong = (owner == chosen) | (owner == (partner + blocks // 2) % blocks)
    return jnp.where(strong, factor * drawn, drawn)


def steps_of(rng, extent, shards, least, high):
    level = 1.0
    for position, parts in shards:
        draws = jax.random.uniform(jax.random.fold_in(jax.random.fold_in(rng, 6), position), (parts,), jnp.float32, least / len(shards), high / len(shards))
        level = level * jnp.repeat(jnp.exp(draws), extent[position] // parts).reshape((-1,) + (1,) * (len(extent) - 1 - position))
    return level


def noise(stream_key, shape, scale, bound, split=(), held_as=jnp.bfloat16):
    factor_of = steps_of(stream_key, shape, split, -0.22, 0.18) if split else 1.0
    entries = jax.random.normal(stream_key, shape, jnp.float32) * scale * factor_of
    return jnp.minimum(jnp.maximum(entries, -bound), bound).astype(held_as)


def bell_draw_with(stream_key, extent, spread, most, shards, heavy, dtype=jnp.bfloat16):
    array = spread * jax.random.normal(stream_key, extent, jnp.float32)
    if shards:
        array = array * steps_of(stream_key, extent, shards, -0.22, 0.18)
    return jnp.clip(strengthened(array, jax.random.fold_in(stream_key, 3), *heavy), -most, most).astype(dtype)


def setup_inputs(seed: int = 0) -> dict:
    arg_keys = jax.random.split(jax.random.key(seed), 5)
    return {
        "latent_raw": bell_draw_with(arg_keys[0], (TOKENS, KVL), 1.0, 6.0, ((0, 32),), (0, 1, 32, 2.75)),
        "norm_gain": jnp.clip(1.0 + 0.1 * jax.random.normal(arg_keys[1], (KVL,), jnp.float32), 0.5, 1.5),
        "up_weight": noise(arg_keys[2], (KVL, HEADS * 2 * HEAD_DIM), KVL ** -0.5, 0.25),
        "grad_kv": noise(arg_keys[3], (TOKENS, HEADS * 2 * HEAD_DIM), 0.5, 3.0, ((0, 32),)),
    }


epsilon = 1e-06

def reference(latent_raw, norm_gain, up_weight, grad_kv):
    latent_full = latent_raw.astype(jnp.float32)
    inverse = lax.rsqrt(lax.optimization_barrier(jnp.mean(latent_full * latent_full, axis=-1, keepdims=True)) + epsilon)
    scaled_rows = latent_full * inverse
    normed = (scaled_rows * norm_gain).astype(jnp.bfloat16)
    factor = float(TOKENS) ** (-0.5)
    grad_norm = lax.dot_general(grad_kv, up_weight, (((1,), (1,)), ((), ())), preferred_element_type=jnp.float32)
    gain_grad = lax.optimization_barrier(jnp.sum(grad_norm * scaled_rows, axis=0)) * factor
    upstream = grad_norm * norm_gain
    centred = upstream - scaled_rows * lax.optimization_barrier(jnp.mean(upstream * scaled_rows, axis=-1, keepdims=True))
    latent_grad = (inverse * centred).astype(jnp.bfloat16)
    weight_grad = lax.dot_general(normed, grad_kv, (((0,), (0,)), ((), ())), preferred_element_type=jnp.float32) * factor
    return (latent_grad, gain_grad, weight_grad)
```

```python
import functools

import jax
import jax.numpy as jnp
from jax import lax
from jax.experimental import pallas as pl
from jax.experimental.pallas import tpu as pltpu
from jax.sharding import PartitionSpec as P

epsilon = 1e-06
MESH = pl.DeviceIdType.MESH
CHUNKS = 4
LAG = 1


def normalize(latent_raw):
    latent_full = latent_raw.astype(jnp.float32)
    inverse = lax.rsqrt(jnp.mean(latent_full * latent_full, axis=-1, keepdims=True) + epsilon)
    return (latent_full * inverse, inverse)


def norm_backward(grad_norm, scaled_rows, inverse, norm_gain):
    upstream = grad_norm * norm_gain
    centred = upstream - scaled_rows * jnp.mean(upstream * scaled_rows, axis=-1, keepdims=True)
    return (inverse * centred).astype(jnp.bfloat16)


def per_device(latent_raw, norm_gain, up_weight, grad_kv):
    scaled_rows, inverse = normalize(latent_raw)
    normed = (scaled_rows * norm_gain).astype(jnp.bfloat16)
    factor = float(latent_raw.shape[0] * lax.axis_size("dp")) ** (-0.5)
    partial_norm = lax.dot_general(
        grad_kv, up_weight, (((1,), (1,)), ((), ())), preferred_element_type=jnp.float32
    )
    grad_norm = lax.psum_scatter(partial_norm, "tensor", scatter_dimension=0, tiled=True)
    row_count = grad_norm.shape[0]
    offset = lax.axis_index("tensor") * row_count
    scaled_part = lax.dynamic_slice_in_dim(scaled_rows, offset, row_count, 0)
    inverse_part = lax.dynamic_slice_in_dim(inverse, offset, row_count, 0)
    gain_local = jnp.sum(grad_norm * scaled_part, axis=0)
    latent_part = norm_backward(grad_norm, scaled_part, inverse_part, norm_gain)
    latent_grad = lax.all_gather(latent_part, "tensor", axis=0, tiled=True)
    gain_grad = lax.psum(gain_local, ("dp", "tensor")) * factor
    weight_partial = lax.dot_general(
        normed, grad_kv, (((0,), (0,)), ((), ())), preferred_element_type=jnp.float32
    )
    weight_grad = lax.psum_scatter(weight_partial, "dp", scatter_dimension=0, tiled=True) * factor
    return (latent_grad, gain_grad, weight_grad)


def kernel(
    planes, factor, latent_ref, gain_ref, weight_hbm, grad_hbm,
    latent_out, gain_out, weight_out,
    own_grad, peer_grad, weight, turned, peer_turned, left,
    send_one, recv_one, keep_one, send_two, recv_two, keep_two,
    send_three, recv_three, keep_three, grad_norm, gain_send, gain_recv,
    load_sem, weight_sem, turned_sem, grad_send_sem, grad_recv_sem,
    one_send_sem, one_recv_sem, two_send_sem, two_recv_sem,
    three_send_sem, three_recv_sem, gain_send_sem, gain_recv_sem,
):
    units, _, width = own_grad.shape
    chunks = units // 2
    rows = weight_out.shape[0]
    me = lax.axis_index("dp")
    core, x, y, z = me % 2, (me // 2) % 2, (me // 4) % 2, me // 8
    partner = me + 1 - 2 * core
    over_x = me + 2 - 4 * x
    over_y = me + 4 - 8 * y
    others = [(z + step) % planes for step in range(1, planes)]
    peers = [partner, over_x, over_y] + [other * 8 + me % 8 for other in others]

    def columns(unit):
        return pl.ds(unit * width, width)

    def send(source, target, send_sem, recv_sem, device):
        return pltpu.make_async_remote_copy(
            src_ref=source, dst_ref=target, send_sem=send_sem, recv_sem=recv_sem,
            device_id={"dp": device}, device_id_type=MESH,
        )

    order = [half * chunks + chunk for chunk in range(chunks) for half in range(2)]
    loads = {}
    for unit in order:
        loads[unit] = pltpu.make_async_copy(
            grad_hbm.at[:, columns(unit)], own_grad.at[unit], load_sem.at[unit]
        )
        loads[unit].start()
    weight_loads = {}
    for unit in order:
        weight_loads[unit] = pltpu.make_async_copy(
            weight_hbm.at[:, columns(unit)], weight.at[unit], weight_sem.at[unit]
        )
        weight_loads[unit].start()

    barrier = pltpu.get_barrier_semaphore()
    for peer in peers:
        pl.semaphore_signal(barrier, inc=1, device_id={"dp": peer}, device_id_type=MESH)

    scaled_rows, _ = normalize(latent_ref[...])
    normed = scaled_rows * gain_ref[...]
    flipped = normed.T.astype(jnp.bfloat16)
    flipped = flipped.reshape(planes * 4, 2, rows, flipped.shape[1])
    turned[0] = flipped[:, 0]
    turned[1] = flipped[:, 1]

    pl.semaphore_wait(barrier, len(peers))

    grads = {}
    for position, unit in enumerate(order):
        loads[unit].wait()
        grads[unit] = send(
            own_grad.at[unit], peer_grad.at[unit],
            grad_send_sem.at[unit], grad_recv_sem.at[unit], partner,
        )
        grads[unit].start()
        if position == 0:
            turned_copy = send(
                turned.at[1 - core], peer_turned, turned_sem.at[0], turned_sem.at[1], partner
            )
            turned_copy.start()

    def block(plane, away_y, away_x):
        to_y = (1 - y) if away_y else y
        to_x = (1 - x) if away_x else x
        return plane * 4 + to_y * 2 + to_x

    def arrange(side, source):
        for first in range(2):
            for second in range(2):
                for plane in range(planes):
                    place = (first * 2 + second) * planes + plane
                    left[0, side, place] = source(block(plane, second == 0, first == 0))
                    left[1, side, place] = source(block(plane, first == 0, second == 0))

    arrange(0, lambda index: turned[core, index])
    turned_copy.wait_recv()
    arrange(1, lambda index: peer_turned[index])

    def left_of(half, side):
        value = left[half, side]
        return value.reshape(planes * 4 * rows, value.shape[-1])

    ones, twos, threes = {}, {}, {}
    half_rows = planes * 2 * rows
    quarter_rows = planes * rows

    def stage_one(unit):
        half = unit // chunks
        grads[unit].wait_recv()
        partial = jnp.dot(
            left_of(half, 0), own_grad[unit], preferred_element_type=jnp.float32
        ) + jnp.dot(left_of(half, 1), peer_grad[unit], preferred_element_type=jnp.float32)
        send_one[unit] = partial[:half_rows].astype(jnp.bfloat16)
        keep_one[unit] = partial[half_rows:]
        ones[unit] = send(
            send_one.at[unit], recv_one.at[unit],
            one_send_sem.at[unit], one_recv_sem.at[unit], over_y if half else over_x,
        )
        ones[unit].start()

    def stage_two(unit):
        half = unit // chunks
        ones[unit].wait_recv()
        total = keep_one[unit] + recv_one[unit].astype(jnp.float32)
        send_two[unit] = total[:quarter_rows].astype(jnp.bfloat16)
        keep_two[unit] = total[quarter_rows:]
        twos[unit] = send(
            send_two.at[unit], recv_two.at[unit],
            two_send_sem.at[unit], two_recv_sem.at[unit], over_x if half else over_y,
        )
        twos[unit].start()

    def stage_three(unit):
        twos[unit].wait_recv()
        total = keep_two[unit] + recv_two[unit].astype(jnp.float32)
        total = total.reshape(planes, rows, width)
        send_three[unit] = total.astype(jnp.bfloat16)
        keep_three[unit] = total
        for index, other in enumerate(others):
            threes[unit, index] = send(
                send_three.at[unit, other], recv_three.at[unit, z],
                three_send_sem.at[unit, other], three_recv_sem.at[unit, z], other * 8 + me % 8,
            )
            threes[unit, index].start()

    def arrival(unit, other):
        return send(
            send_three.at[unit, other], recv_three.at[unit, other],
            three_send_sem.at[unit, other], three_recv_sem.at[unit, other], other * 8 + me % 8,
        )

    def finish(unit):
        total = keep_three[unit, z]
        for other in others:
            arrival(unit, other).wait_recv()
            total = total + recv_three[unit, other].astype(jnp.float32)
        weight_out[:, columns(unit)] = total * factor

    def norm_part(unit, first):
        weight_loads[unit].wait()
        product = lax.dot_general(
            own_grad[unit], weight[unit], (((1,), (1,)), ((), ())),
            preferred_element_type=jnp.float32,
        )
        grad_norm[...] = product if first else grad_norm[...] + product

    gains = []

    def gain_exchange(stage, value, device):
        gain_send[stage] = value
        copy = send(
            gain_send.at[stage], gain_recv.at[stage],
            gain_send_sem.at[stage], gain_recv_sem.at[stage], device,
        )
        copy.start()
        gains.append(copy)

    def gain_take(stage):
        gains[stage].wait_recv()
        return gain_send[stage] + gain_recv[stage]

    def norm_rest():
        scaled, inverse = normalize(latent_ref[...])
        grads_here = grad_norm[...]
        gain_exchange(0, jnp.sum(grads_here * scaled, axis=0, keepdims=True), partner)
        latent_out[...] = norm_backward(grads_here, scaled, inverse, gain_ref[...])

    def both(stage, chunk):
        if 0 <= chunk < chunks:
            stage(chunk)
            stage(chunks + chunk)

    for turn in range(chunks + 3 * LAG):
        both(stage_one, turn)
        if turn == chunks - 1:
            for position, unit in enumerate(order):
                norm_part(unit, position == 0)
            norm_rest()
        both(stage_two, turn - LAG)
        if turn == chunks:
            gain_exchange(1, gain_take(0), over_x)
        both(stage_three, turn - 2 * LAG)
        if turn == chunks + LAG:
            gain_exchange(2, gain_take(1), over_y)
        both(finish, turn - 3 * LAG)

    total_gain = gain_take(2)
    gain_send[3] = total_gain
    gain_recv[3 + z] = total_gain
    last = []
    for index, other in enumerate(others):
        copy = send(
            gain_send.at[3], gain_recv.at[3 + z],
            gain_send_sem.at[3 + index], gain_recv_sem.at[3 + z], other * 8 + me % 8,
        )
        copy.start()
        last.append(copy)
    for index, other in enumerate(others):
        send(
            gain_send.at[3], gain_recv.at[3 + other],
            gain_send_sem.at[3 + index], gain_recv_sem.at[3 + other], other * 8 + me % 8,
        ).wait_recv()
    total_gain = gain_recv[3]
    for plane in range(1, planes):
        total_gain = total_gain + gain_recv[3 + plane]
    gain_out[...] = total_gain * factor

    turned_copy.wait_send()
    for group in (grads, ones, twos, threes):
        for copy in group.values():
            copy.wait_send()
    for copy in gains + last:
        copy.wait_send()


def fused(latent_raw, norm_gain, up_weight, grad_kv):
    devices = lax.axis_size("dp")
    planes = devices // 8
    tokens, latent_width = latent_raw.shape
    total_columns = grad_kv.shape[1]
    units = 2 * CHUNKS
    width = total_columns // units
    rows = latent_width // devices
    factor = float(tokens * devices) ** (-0.5)
    half_rows, quarter_rows = planes * 2 * rows, planes * rows
    bf16, f32 = jnp.bfloat16, jnp.float32
    dma = pltpu.SemaphoreType.DMA
    vmem = pl.BlockSpec(memory_space=pltpu.VMEM)
    hbm = pl.BlockSpec(memory_space=pl.ANY)
    latent_grad, gain_grad, weight_grad = pl.pallas_call(
        functools.partial(kernel, planes, factor),
        out_shape=(
            jax.ShapeDtypeStruct((tokens, latent_width), bf16),
            jax.ShapeDtypeStruct((1, latent_width), f32),
            jax.ShapeDtypeStruct((rows, total_columns), f32),
        ),
        in_specs=[vmem, vmem, hbm, hbm],
        out_specs=(vmem, vmem, vmem),
        scratch_shapes=[
            pltpu.VMEM((units, tokens, width), bf16),
            pltpu.VMEM((units, tokens, width), bf16),
            pltpu.VMEM((units, latent_width, width), bf16),
            pltpu.VMEM((2, planes * 4, rows, tokens), bf16),
            pltpu.VMEM((planes * 4, rows, tokens), bf16),
            pltpu.VMEM((2, 2, planes * 4, rows, tokens), bf16),
            pltpu.VMEM((units, half_rows, width), bf16),
            pltpu.VMEM((units, half_rows, width), bf16),
            pltpu.VMEM((units, half_rows, width), f32),
            pltpu.VMEM((units, quarter_rows, width), bf16),
            pltpu.VMEM((units, quarter_rows, width), bf16),
            pltpu.VMEM((units, quarter_rows, width), f32),
            pltpu.VMEM((units, planes, rows, width), bf16),
            pltpu.VMEM((units, planes, rows, width), bf16),
            pltpu.VMEM((units, planes, rows, width), f32),
            pltpu.VMEM((tokens, latent_width), f32),
            pltpu.VMEM((4, 1, latent_width), f32),
            pltpu.VMEM((3 + planes, 1, latent_width), f32),
            dma((units,)), dma((units,)), dma((2,)), dma((units,)), dma((units,)),
            dma((units,)), dma((units,)), dma((units,)), dma((units,)),
            dma((units, planes)), dma((units, planes)),
            dma((3 + planes,)), dma((3 + planes,)),
        ],
        compiler_params=pltpu.CompilerParams(
            collective_id=0, has_side_effects=True, vmem_limit_bytes=48 * 1024 * 1024
        ),
    )(latent_raw, norm_gain.reshape(1, latent_width), up_weight, grad_kv)
    return (latent_grad, gain_grad.reshape(latent_width), weight_grad)


def solution(mesh):
    devices = mesh.shape["dp"]
    covered = mesh.shape["tensor"] == 1 and devices % 8 == 0 and 16 <= devices <= 32
    in_specs = (P("dp", None), P(), P(None, "tensor"), P("dp", "tensor"))
    out_specs = (P("dp", None), P(), P("dp", "tensor"))
    return jax.shard_map(
        fused if covered else per_device,
        mesh=mesh, in_specs=in_specs, out_specs=out_specs, check_vma=False,
    )
```

```python
import functools

import jax
import jax.numpy as jnp
from jax import lax
from jax.experimental import pallas as pl
from jax.experimental.pallas import tpu as pltpu
from jax.sharding import PartitionSpec as P

epsilon = 1e-06
MESH = pl.DeviceIdType.MESH
CHUNKS = 4
LAG = 1
NORM_TURN = 1
GAIN_STEP = 1


def normalize(latent_raw):
    latent_full = latent_raw.astype(jnp.float32)
    inverse = lax.rsqrt(jnp.mean(latent_full * latent_full, axis=-1, keepdims=True) + epsilon)
    return (latent_full * inverse, inverse)


def norm_backward(grad_norm, scaled_rows, inverse, norm_gain):
    upstream = grad_norm * norm_gain
    centred = upstream - scaled_rows * jnp.mean(upstream * scaled_rows, axis=-1, keepdims=True)
    return (inverse * centred).astype(jnp.bfloat16)


def per_device(latent_raw, norm_gain, up_weight, grad_kv):
    scaled_rows, inverse = normalize(latent_raw)
    normed = (scaled_rows * norm_gain).astype(jnp.bfloat16)
    factor = float(latent_raw.shape[0] * lax.axis_size("dp")) ** (-0.5)
    partial_norm = lax.dot_general(
        grad_kv, up_weight, (((1,), (1,)), ((), ())), preferred_element_type=jnp.float32
    )
    grad_norm = lax.psum_scatter(partial_norm, "tensor", scatter_dimension=0, tiled=True)
    row_count = grad_norm.shape[0]
    offset = lax.axis_index("tensor") * row_count
    scaled_part = lax.dynamic_slice_in_dim(scaled_rows, offset, row_count, 0)
    inverse_part = lax.dynamic_slice_in_dim(inverse, offset, row_count, 0)
    gain_local = jnp.sum(grad_norm * scaled_part, axis=0)
    latent_part = norm_backward(grad_norm, scaled_part, inverse_part, norm_gain)
    latent_grad = lax.all_gather(latent_part, "tensor", axis=0, tiled=True)
    gain_grad = lax.psum(gain_local, ("dp", "tensor")) * factor
    weight_partial = lax.dot_general(
        normed, grad_kv, (((0,), (0,)), ((), ())), preferred_element_type=jnp.float32
    )
    weight_grad = lax.psum_scatter(weight_partial, "dp", scatter_dimension=0, tiled=True) * factor
    return (latent_grad, gain_grad, weight_grad)


def kernel(
    planes, factor, latent_hbm, gain_hbm, weight_hbm, grad_hbm,
    latent_out, gain_out, weight_out, latent_ref, gain_ref,
    own_grad, peer_grad, weight, turned, peer_turned, left,
    send_one, recv_one, keep_one, send_two, recv_two, keep_two,
    send_three, recv_three, keep_three, grad_norm, gain_send, gain_recv,
    small_sem, load_sem, weight_sem, turned_sem, grad_send_sem, grad_recv_sem,
    one_send_sem, one_recv_sem, two_send_sem, two_recv_sem,
    three_send_sem, three_recv_sem, gain_send_sem, gain_recv_sem,
):
    units, _, width = own_grad.shape
    chunks = units // 2
    rows = weight_out.shape[0]
    me = lax.axis_index("dp")
    core, x, y, z = me % 2, (me // 2) % 2, (me // 4) % 2, me // 8
    partner = me + 1 - 2 * core
    over_x = me + 2 - 4 * x
    over_y = me + 4 - 8 * y
    others = [(z + step) % planes for step in range(1, planes)]
    peers = [partner, over_x, over_y] + [other * 8 + me % 8 for other in others]

    def columns(unit):
        return pl.ds(unit * width, width)

    def send(source, target, send_sem, recv_sem, device):
        return pltpu.make_async_remote_copy(
            src_ref=source, dst_ref=target, send_sem=send_sem, recv_sem=recv_sem,
            device_id={"dp": device}, device_id_type=MESH,
        )

    small_loads = [
        pltpu.make_async_copy(latent_hbm, latent_ref, small_sem.at[0]),
        pltpu.make_async_copy(gain_hbm, gain_ref, small_sem.at[1]),
    ]
    for copy in small_loads:
        copy.start()
    order = [half * chunks + chunk for chunk in range(chunks) for half in range(2)]
    loads = {}
    for unit in order:
        loads[unit] = pltpu.make_async_copy(
            grad_hbm.at[:, columns(unit)], own_grad.at[unit], load_sem.at[unit]
        )
        loads[unit].start()
    weight_loads = {}
    for unit in order:
        weight_loads[unit] = pltpu.make_async_copy(
            weight_hbm.at[:, columns(unit)], weight.at[unit], weight_sem.at[unit]
        )
        weight_loads[unit].start()

    barrier = pltpu.get_barrier_semaphore()
    for peer in peers:
        pl.semaphore_signal(barrier, inc=1, device_id={"dp": peer}, device_id_type=MESH)

    for copy in small_loads:
        copy.wait()
    scaled_rows, _ = normalize(latent_ref[...])
    normed = scaled_rows * gain_ref[...]
    flipped = normed.T.astype(jnp.bfloat16)
    flipped = flipped.reshape(planes * 4, 2, rows, flipped.shape[1])
    turned[0] = flipped[:, 0]
    turned[1] = flipped[:, 1]

    pl.semaphore_wait(barrier, len(peers))

    grads = {}
    for position, unit in enumerate(order):
        loads[unit].wait()
        grads[unit] = send(
            own_grad.at[unit], peer_grad.at[unit],
            grad_send_sem.at[unit], grad_recv_sem.at[unit], partner,
        )
        grads[unit].start()
        if position == 0:
            turned_copy = send(
                turned.at[1 - core], peer_turned, turned_sem.at[0], turned_sem.at[1], partner
            )
            turned_copy.start()

    def block(plane, away_y, away_x):
        to_y = (1 - y) if away_y else y
        to_x = (1 - x) if away_x else x
        return plane * 4 + to_y * 2 + to_x

    def arrange(side, source):
        for first in range(2):
            for second in range(2):
                for plane in range(planes):
                    place = (first * 2 + second) * planes + plane
                    left[0, side, place] = source(block(plane, second == 0, first == 0))
                    left[1, side, place] = source(block(plane, first == 0, second == 0))

    arrange(0, lambda index: turned[core, index])
    turned_copy.wait_recv()
    arrange(1, lambda index: peer_turned[index])

    def left_of(half, side):
        value = left[half, side]
        return value.reshape(planes * 4 * rows, value.shape[-1])

    ones, twos, threes = {}, {}, {}
    half_rows = planes * 2 * rows
    quarter_rows = planes * rows

    def stage_one(unit):
        half = unit // chunks
        grads[unit].wait_recv()
        partial = jnp.dot(
            left_of(half, 0), own_grad[unit], preferred_element_type=jnp.float32
        ) + jnp.dot(left_of(half, 1), peer_grad[unit], preferred_element_type=jnp.float32)
        send_one[unit] = partial[:half_rows].astype(jnp.bfloat16)
        keep_one[unit] = partial[half_rows:]
        ones[unit] = send(
            send_one.at[unit], recv_one.at[unit],
            one_send_sem.at[unit], one_recv_sem.at[unit], over_y if half else over_x,
        )
        ones[unit].start()

    def stage_two(unit):
        half = unit // chunks
        ones[unit].wait_recv()
        total = keep_one[unit] + recv_one[unit].astype(jnp.float32)
        send_two[unit] = total[:quarter_rows].astype(jnp.bfloat16)
        keep_two[unit] = total[quarter_rows:]
        twos[unit] = send(
            send_two.at[unit], recv_two.at[unit],
            two_send_sem.at[unit], two_recv_sem.at[unit], over_x if half else over_y,
        )
        twos[unit].start()

    def stage_three(unit):
        twos[unit].wait_recv()
        total = keep_two[unit] + recv_two[unit].astype(jnp.float32)
        total = total.reshape(planes, rows, width)
        send_three[unit] = total.astype(jnp.bfloat16)
        keep_three[unit] = total
        for index, other in enumerate(others):
            threes[unit, index] = send(
                send_three.at[unit, other], recv_three.at[unit, z],
                three_send_sem.at[unit, other], three_recv_sem.at[unit, z], other * 8 + me % 8,
            )
            threes[unit, index].start()

    def arrival(unit, other):
        return send(
            send_three.at[unit, other], recv_three.at[unit, other],
            three_send_sem.at[unit, other], three_recv_sem.at[unit, other], other * 8 + me % 8,
        )

    def finish(unit):
        total = keep_three[unit, z]
        for other in others:
            arrival(unit, other).wait_recv()
            total = total + recv_three[unit, other].astype(jnp.float32)
        weight_out[:, columns(unit)] = total * factor

    def norm_part(unit, first):
        weight_loads[unit].wait()
        product = lax.dot_general(
            own_grad[unit], weight[unit], (((1,), (1,)), ((), ())),
            preferred_element_type=jnp.float32,
        )
        grad_norm[...] = product if first else grad_norm[...] + product

    gains = []

    def gain_send_to(stage, slot, device, at):
        copy = send(
            gain_send.at[stage], gain_recv.at[slot],
            gain_send_sem.at[at], gain_recv_sem.at[slot], device,
        )
        copy.start()
        gains.append(copy)

    def gain_pair(stage, device):
        gain_send_to(stage, stage, device, stage)

    def gain_take(stage):
        gains_of[stage].wait_recv()
        return gain_send[stage] + gain_recv[stage]

    gains_of = {}

    def gain_first(value):
        gain_send[0] = value
        gain_pair(0, partner)
        gains_of[0] = gains[-1]

    def gain_planes():
        value = gain_take(0)
        gain_send[3] = value
        gain_recv[3 + z] = value
        for index, other in enumerate(others):
            gain_send_to(3, 3 + z, other * 8 + me % 8, 3 + index)

    def gain_over_x():
        for index, other in enumerate(others):
            send(
                gain_send.at[3], gain_recv.at[3 + other],
                gain_send_sem.at[3 + index], gain_recv_sem.at[3 + other], other * 8 + me % 8,
            ).wait_recv()
        value = gain_recv[3]
        for plane in range(1, planes):
            value = value + gain_recv[3 + plane]
        gain_send[1] = value
        gain_pair(1, over_x)
        gains_of[1] = gains[-1]

    def gain_over_y():
        gain_send[2] = gain_take(1)
        gain_pair(2, over_y)
        gains_of[2] = gains[-1]

    def gain_end():
        gain_out[...] = gain_take(2) * factor

    def norm_rest():
        scaled, inverse = normalize(latent_ref[...])
        grads_here = grad_norm[...]
        gain_first(jnp.sum(grads_here * scaled, axis=0, keepdims=True))
        latent_out[...] = norm_backward(grads_here, scaled, inverse, gain_ref[...])

    def both(stage, chunk):
        if 0 <= chunk < chunks:
            stage(chunk)
            stage(chunks + chunk)

    for turn in range(chunks + 3 * LAG):
        both(stage_one, turn)
        if turn == NORM_TURN:
            for position, unit in enumerate(order):
                norm_part(unit, position == 0)
            norm_rest()
        both(stage_two, turn - LAG)
        if turn == NORM_TURN:
            gain_planes()
        both(stage_three, turn - 2 * LAG)
        if turn == NORM_TURN + GAIN_STEP:
            gain_over_x()
        if turn == NORM_TURN + 2 * GAIN_STEP:
            gain_over_y()
        if turn == NORM_TURN + 3 * GAIN_STEP:
            gain_end()
        both(finish, turn - 3 * LAG)

    turned_copy.wait_send()
    for group in (grads, ones, twos, threes):
        for copy in group.values():
            copy.wait_send()
    for copy in gains:
        copy.wait_send()


def place_kernel(first_in, second_in, third_in, first_out, second_out, third_out, sem):
    pairs = ((first_in, first_out), (second_in, second_out), (third_in, third_out))
    copies = [pltpu.make_async_copy(*pair, sem.at[at]) for at, pair in enumerate(pairs)]
    for copy in copies:
        copy.start()
    for copy in copies:
        copy.wait()


def place(*arrays):
    hbm = pl.BlockSpec(memory_space=pl.ANY)
    vmem = pl.BlockSpec(memory_space=pltpu.VMEM)
    return pl.pallas_call(
        place_kernel,
        out_shape=tuple(jax.ShapeDtypeStruct(a.shape, a.dtype) for a in arrays),
        in_specs=[vmem] * 3,
        out_specs=(hbm,) * 3,
        scratch_shapes=[pltpu.SemaphoreType.DMA((3,))],
        compiler_params=pltpu.CompilerParams(vmem_limit_bytes=8 * 1024 * 1024),
    )(*arrays)


def fused(latent_raw, norm_gain, up_weight, grad_kv):
    devices = lax.axis_size("dp")
    planes = devices // 8
    tokens, latent_width = latent_raw.shape
    total_columns = grad_kv.shape[1]
    units = 2 * CHUNKS
    width = total_columns // units
    rows = latent_width // devices
    factor = float(tokens * devices) ** (-0.5)
    half_rows, quarter_rows = planes * 2 * rows, planes * rows
    bf16, f32 = jnp.bfloat16, jnp.float32
    dma = pltpu.SemaphoreType.DMA
    vmem = pl.BlockSpec(memory_space=pltpu.VMEM)
    hbm = pl.BlockSpec(memory_space=pl.ANY)
    latent_grad, gain_grad, weight_grad = pl.pallas_call(
        functools.partial(kernel, planes, factor),
        out_shape=(
            pltpu.VMEM((tokens, latent_width), bf16),
            pltpu.VMEM((1, latent_width), f32),
            pltpu.VMEM((rows, total_columns), f32),
        ),
        in_specs=[pl.BlockSpec(memory_space=pltpu.HBM)] * 4,
        out_specs=(vmem, vmem, vmem),
        scratch_shapes=[
            pltpu.VMEM((tokens, latent_width), bf16),
            pltpu.VMEM((1, latent_width), f32),
            pltpu.VMEM((units, tokens, width), bf16),
            pltpu.VMEM((units, tokens, width), bf16),
            pltpu.VMEM((units, latent_width, width), bf16),
            pltpu.VMEM((2, planes * 4, rows, tokens), bf16),
            pltpu.VMEM((planes * 4, rows, tokens), bf16),
            pltpu.VMEM((2, 2, planes * 4, rows, tokens), bf16),
            pltpu.VMEM((units, half_rows, width), bf16),
            pltpu.VMEM((units, half_rows, width), bf16),
            pltpu.VMEM((units, half_rows, width), f32),
            pltpu.VMEM((units, quarter_rows, width), bf16),
            pltpu.VMEM((units, quarter_rows, width), bf16),
            pltpu.VMEM((units, quarter_rows, width), f32),
            pltpu.VMEM((units, planes, rows, width), bf16),
            pltpu.VMEM((units, planes, rows, width), bf16),
            pltpu.VMEM((units, planes, rows, width), f32),
            pltpu.VMEM((tokens, latent_width), f32),
            pltpu.VMEM((4, 1, latent_width), f32),
            pltpu.VMEM((3 + planes, 1, latent_width), f32),
            dma((2,)), dma((units,)), dma((units,)), dma((2,)), dma((units,)), dma((units,)),
            dma((units,)), dma((units,)), dma((units,)), dma((units,)),
            dma((units, planes)), dma((units, planes)),
            dma((3 + planes,)), dma((3 + planes,)),
        ],
        compiler_params=pltpu.CompilerParams(
            collective_id=0, has_side_effects=True, vmem_limit_bytes=67043328 - 512 * 1024
        ),
    )(latent_raw, norm_gain.reshape(1, latent_width), up_weight, grad_kv)
    latent_grad, gain_grad, weight_grad = place(latent_grad, gain_grad, weight_grad)
    return (latent_grad, gain_grad.reshape(latent_width), weight_grad)


def solution(mesh):
    devices = mesh.shape["dp"]
    covered = mesh.shape["tensor"] == 1 and devices % 8 == 0 and 16 <= devices <= 32
    in_specs = (P("dp", None), P(), P(None, "tensor"), P("dp", "tensor"))
    out_specs = (P("dp", None), P(), P("dp", "tensor"))
    return jax.shard_map(
        fused if covered else per_device,
        mesh=mesh, in_specs=in_specs, out_specs=out_specs, check_vma=False,
    )
```
